32 devices in a mesh: dp: 8 (over z, y), tensor: 4 (over x, core).
Axes of the slice: x: 2, y: 2, z: 4, core: 2. Of those that a mesh axis runs over, the one named last changes fastest.
Arguments:
- hidden: bfloat16 [2048, 18432], P('dp', 'tensor'), may hold values from -6 to 6
- down_weight: bfloat16 [18432, 4608], P('tensor', 'dp'), may hold values from -0.046875 to 0.046875
- residual: bfloat16 [2048, 4608], P('dp'), may hold values from -6 to 6
- post_gain: float32 [4608], replicated, may hold values from 0.5 to 1.5
- pre_gain: float32 [4608], replicated, may hold values from 0.5 to 1.5
- cast_scale: float32 [1], replicated, may hold values from 100 to 400
- amax_history: float32 [3, 1024], replicated, may hold values from 0.25 to 4
Outputs:
- cast_out: bfloat16 [2048, 4608], P('dp')
- residual_out: bfloat16 [2048, 4608], P('dp')
- peaks: float32 [3], replicated
- new_history: float32 [3, 1024], replicated
- new_scales: float32 [3], replicated
The draws below stay inside these ranges and needn't reach their ends.
All inputs are finite; a program needn't handle non-finite values.
Results may differ from the reference program's by a relative error of at most 0.012.
Values may be sent and summed in bfloat16 or wider, within the bound.
No kernel may reach another device: no remote copies, remote signals or barrier semaphores. Data moves between devices by JAX's collectives and lax.ppermute only.
A program may use at most 128 MiB of HBM per device.

```python
import math
import jax
import jax.numpy as jnp
from jax import lax

D = 4608
FF_WIN = 18432
HIST = 1024
FF_DEV = 4608
TOKENS = 2048


def block_scale(key, shape, split, low, top_value):
    gain, own = 1.0, jax.random.fold_in(key, 6)
    for dim, shards_of in split:
        heights = jnp.exp(jax.random.uniform(jax.random.fold_in(own, dim), (shards_of,), jnp.float32, low / len(split), top_value / len(split)))
        gain = gain * jnp.repeat(heights, shape[dim] // shards_of).reshape([-1 if axis == dim else 1 for axis in range(len(shape))])
    return gain


def centred(own_key, dims, scale, most, pieces=(), kind=jnp.bfloat16):
    loudness = block_scale(own_key, dims, pieces, -0.22, 0.18) if pieces else 1.0
    array = jax.random.normal(own_key, dims, jnp.float32) * scale * loudness
    return jnp.minimum(jnp.maximum(array, -most), most).astype(kind)


def setup_inputs(seed: int = 0) -> dict:
    key_list = jax.random.split(jax.random.key(seed), 8)
    hidden = centred(key_list[0], (TOKENS, FF_WIN), 1.0, 6.0, ((0, 8), (1, 4)))
    down_weight = centred(key_list[1], (FF_WIN, D), FF_WIN ** -0.5, 0.046875, ((0, 4), (1, 8)))
    residual = centred(key_list[2], (TOKENS, D), 1.0, 6.0, ((0, 8),))
    post_gain = jnp.clip(1.0 + 0.1 * jax.random.normal(key_list[3], (D,), jnp.float32), 0.5, 1.5)
    pre_gain = jnp.clip(1.0 + 0.1 * jax.random.normal(key_list[4], (D,), jnp.float32), 0.5, 1.5)
    cast_scale = jnp.clip(jnp.exp(jax.random.uniform(key_list[5], (1,), jnp.float32, math.log(100.0), math.log(400.0))), 100.0, 400.0)
    amax_history = jnp.clip(jnp.exp(jax.random.uniform(key_list[6], (3, HIST), jnp.float32, math.log(0.25), math.log(4.0))), 0.25, 4.0)
    return dict(hidden=hidden, down_weight=down_weight, residual=residual, post_gain=post_gain, pre_gain=pre_gain, cast_scale=cast_scale, amax_history=amax_history)


norm_epsilon = 1e-06
float_limit = 448.0

def rms_norm(values, gain_vector):
    return values * lax.rsqrt(lax.optimization_barrier(jnp.mean(values * values, axis=-1, keepdims=True)) + norm_epsilon) * gain_vector

def reference(hidden, down_weight, residual, post_gain, pre_gain, cast_scale, amax_history):
    summed = jnp.zeros((hidden.shape[0], down_weight.shape[1]), jnp.float32)
    for shard_index in range(FF_WIN // FF_DEV):
        first = shard_index * FF_DEV
        term = jnp.dot(hidden[:, first:first + FF_DEV], down_weight[first:first + FF_DEV, :], preferred_element_type=jnp.float32)
        term = lax.optimization_barrier(term.astype(jnp.bfloat16)).astype(jnp.float32)
        summed = summed + term
    stream = residual.astype(jnp.float32) + rms_norm(summed, post_gain)
    normed = rms_norm(stream, pre_gain)
    stale_scale = cast_scale[0]
    cast_out = (jnp.clip(normed * stale_scale, -float_limit, float_limit) / stale_scale).astype(jnp.bfloat16)
    peak_values = jnp.stack([jnp.max(jnp.abs(summed)), jnp.max(jnp.abs(stream)), jnp.max(jnp.abs(normed))]).astype(jnp.float32)
    new_history = jnp.concatenate([peak_values[:, None], amax_history[:, :-1]], axis=1)
    new_scales = float_limit / jnp.maximum(lax.optimization_barrier(jnp.max(new_history, axis=1)), 1.0)
    return (cast_out, stream.astype(jnp.bfloat16), peak_values, new_history, new_scales)
```

```python
import functools

import jax
import jax.numpy as jnp
from jax import lax
from jax.experimental import pallas as pl
from jax.experimental.pallas import tpu as pltpu
from jax.sharding import PartitionSpec as P

norm_epsilon = 1e-06
float_limit = 448.0
LANES = 128
ROW_STEP = 16
ANY = pl.ANY
VMEM_LIMIT = 60 * 1024 * 1024


def rms_norm(values, gain_vector):
    return (
        values
        * lax.rsqrt(jnp.mean(values * values, axis=-1, keepdims=True) + norm_epsilon)
        * gain_vector
    )


def finish(summed, stream_in, post_gain, pre_gain, stale_scale):
    stream = stream_in.astype(jnp.float32) + rms_norm(summed, post_gain)
    normed = rms_norm(stream, pre_gain)
    cast_rows = (jnp.clip(normed * stale_scale, -float_limit, float_limit) / stale_scale).astype(
        jnp.bfloat16
    )
    peak_values = jnp.stack(
        [jnp.max(jnp.abs(summed)), jnp.max(jnp.abs(stream)), jnp.max(jnp.abs(normed))]
    )
    return (cast_rows, stream.astype(jnp.bfloat16), peak_values)


def histories(peak_values, amax_history):
    new_history = jnp.concatenate([peak_values[:, None], amax_history[:, :-1]], axis=1)
    new_scales = float_limit / jnp.maximum(jnp.max(new_history, axis=1), 1.0)
    return new_history, new_scales


def general(hidden, down_weight, residual, post_gain, pre_gain, cast_scale, amax_history):
    partial_value = jnp.dot(
        lax.all_gather(hidden, "dp", axis=0, tiled=True),
        down_weight,
        preferred_element_type=jnp.float32,
    )
    column_total = lax.psum(partial_value.astype(jnp.bfloat16), "tensor")
    summed = lax.all_to_all(
        column_total, "dp", split_axis=0, concat_axis=1, tiled=True
    ).astype(jnp.float32)
    cast_out, residual_out, peak_values = finish(
        summed, residual, post_gain, pre_gain, cast_scale[0]
    )
    peak_values = lax.pmax(peak_values, ("dp", "tensor"))
    new_history, new_scales = histories(peak_values, amax_history)
    return (cast_out, residual_out, peak_values, new_history, new_scales)


def matmul_kernel(n, nt, where_ref, *refs):
    own_w, other_w, own_h = refs[:3]
    ups, downs = refs[3 : 2 + n], refs[2 + n : 1 + 2 * n]
    out, w_buf, h_buf, o_buf, w_sem, h_sem, o_sem = refs[1 + 2 * n :]
    line, pair, member = where_ref[0], where_ref[1], where_ref[2]
    half = own_w.shape[0]
    rows = own_h.shape[0]
    piece = rows // nt

    def w_copy(src, place, k):
        return pltpu.make_async_copy(
            src, w_buf.at[pl.ds(pl.multiple_of(place * half, half), half)], w_sem.at[k]
        )

    def h_copy(src, r):
        return pltpu.make_async_copy(src, h_buf.at[r % 2], h_sem.at[r % 2])

    def fetch(r):
        @pl.when(line == r)
        def _():
            h_copy(own_h, r).start()

        for s in range(1, n):

            @pl.when(line + s == r)
            def _():
                h_copy(ups[s - 1], r).start()

            @pl.when(line - s == r)
            def _():
                h_copy(downs[s - 1], r).start()

    def o_copies(r):
        found = []
        for k in range(nt):
            place = pl.multiple_of((member ^ k) * piece, piece)
            found.append(
                pltpu.make_async_copy(
                    o_buf.at[r % 2, pl.ds(place, piece)], out.at[k, r], o_sem.at[r % 2, k]
                )
            )
        return found

    w_copy(own_w, pair, 0).start()
    w_copy(other_w, 1 - pair, 1).start()
    fetch(0)
    w_copy(own_w, pair, 0).wait()
    w_copy(other_w, 1 - pair, 1).wait()
    for r in range(n):
        if r + 1 < n:
            fetch(r + 1)
        h_copy(own_h, r).wait()
        if r >= 2:
            for copy in o_copies(r - 2):
                copy.wait()
        o_buf[r % 2] = lax.dot_general(
            h_buf[r % 2],
            w_buf[...],
            (((1,), (1,)), ((), ())),
            preferred_element_type=jnp.float32,
        ).astype(jnp.bfloat16)
        for copy in o_copies(r):
            copy.start()
    for r in range(max(n - 2, 0), n):
        for copy in o_copies(r):
            copy.wait()


def multiply(where, own_w, other_w, own_h, ups, downs, n, nt):
    rows, depth = own_h.shape
    columns = 2 * own_w.shape[0]
    return pl.pallas_call(
        functools.partial(matmul_kernel, n, nt),
        out_shape=jax.ShapeDtypeStruct((nt, n, rows // nt, columns), jnp.bfloat16),
        in_specs=[pl.BlockSpec(memory_space=pltpu.SMEM)]
        + [pl.BlockSpec(memory_space=ANY)] * (3 + 2 * (n - 1)),
        out_specs=pl.BlockSpec(memory_space=ANY),
        scratch_shapes=[
            pltpu.VMEM((columns, depth), jnp.bfloat16),
            pltpu.VMEM((2, rows, depth), jnp.bfloat16),
            pltpu.VMEM((2, rows, columns), jnp.bfloat16),
            pltpu.SemaphoreType.DMA((2,)),
            pltpu.SemaphoreType.DMA((2,)),
            pltpu.SemaphoreType.DMA((2, nt)),
        ],
        compiler_params=pltpu.CompilerParams(vmem_limit_bytes=VMEM_LIMIT),
        cost_estimate=pl.CostEstimate(
            flops=2 * n * rows * depth * columns,
            bytes_accessed=2 * (n * rows + columns) * depth,
            transcendentals=0,
        ),
        name="multiply",
    )(where, own_w, other_w, own_h, *ups, *downs)


def norm_kernel(n, nt, where_ref, scale_ref, residual, post_ref, pre_ref, *refs):
    pieces = refs[:nt]
    cast_out, stream_out, peaks_ref = refs[nt : nt + 3]
    q_buf, r_buf, c_buf, s_buf, t_buf, in_sem, r_sem, c_sem, s_sem = refs[nt + 3 :]
    line, member = where_ref[0], where_ref[2]
    piece, block = q_buf.shape[2], q_buf.shape[3]
    width = n * block
    scale = scale_ref[0]
    slices = [pl.ds(j * LANES, LANES) for j in range(block // LANES)]

    def row_place(k):
        return pl.ds(pl.multiple_of((member ^ k) * piece, piece), piece)

    def in_copy(k):
        return pltpu.make_async_copy(pieces[k], q_buf.at[k % 2], in_sem.at[k % 2])

    def column(i):
        return lax.rem(line - i + n, n)

    def res_copy(k, i):
        place = pl.ds(pl.multiple_of(column(i) * block, block), block)
        return pltpu.make_async_copy(
            residual.at[row_place(k), place], r_buf.at[k % 2, i], r_sem.at[k % 2, i]
        )

    def out_copies(k, i):
        place = pl.ds(pl.multiple_of(column(i) * block, block), block)
        return (
            pltpu.make_async_copy(
                c_buf.at[k % 2, i], cast_out.at[row_place(k), place], c_sem.at[k % 2, i]
            ),
            pltpu.make_async_copy(
                s_buf.at[k % 2, i], stream_out.at[row_place(k), place], s_sem.at[k % 2, i]
            ),
        )

    def start_in(k):
        in_copy(k).start()
        for i in range(n):
            res_copy(k, i).start()

    zero = jnp.zeros((ROW_STEP, LANES), jnp.float32)
    tops = (zero, zero, zero)
    start_in(0)
    for k in range(nt):
        if k + 1 < nt:
            start_in(k + 1)
        in_copy(k).wait()
        for i in range(n):
            res_copy(k, i).wait()
        if k >= 2:
            for i in range(n):
                for copy in out_copies(k - 2, i):
                    copy.wait()
        slot = k % 2

        def step(index, carry, slot=slot):
            top_a, top_b, top_c = carry
            here = pl.ds(pl.multiple_of(index * ROW_STEP, ROW_STEP), ROW_STEP)
            total = zero
            for i in range(n):
                for lanes in slices:
                    v = q_buf[slot, i, here, lanes].astype(jnp.float32)
                    total = total + v * v
                    top_a = jnp.maximum(top_a, jnp.abs(v))
            inverse = lax.rsqrt(jnp.sum(total, axis=-1, keepdims=True) / width + norm_epsilon)
            total = zero
            for i in range(n):
                for lanes in slices:
                    v = q_buf[slot, i, here, lanes].astype(jnp.float32)
                    gain = post_ref[column(i), :, lanes]
                    v = r_buf[slot, i, here, lanes].astype(jnp.float32) + v * inverse * gain
                    t_buf[i, :, lanes] = v
                    s_buf[slot, i, here, lanes] = v.astype(jnp.bfloat16)
                    total = total + v * v
                    top_b = jnp.maximum(top_b, jnp.abs(v))
            inverse = lax.rsqrt(jnp.sum(total, axis=-1, keepdims=True) / width + norm_epsilon)
            for i in range(n):
                for lanes in slices:
                    gain = pre_ref[column(i), :, lanes]
                    v = t_buf[i, :, lanes] * inverse * gain
                    top_c = jnp.maximum(top_c, jnp.abs(v))
                    v = jnp.clip(v * scale, -float_limit, float_limit) / scale
                    c_buf[slot, i, here, lanes] = v.astype(jnp.bfloat16)
            return top_a, top_b, top_c

        tops = lax.fori_loop(0, piece // ROW_STEP, step, tops)
        for i in range(n):
            for copy in out_copies(k, i):
                copy.start()
    for a in range(3):
        peaks_ref[a] = jnp.broadcast_to(jnp.max(tops[a]), peaks_ref.shape[1:])
    for k in range(max(nt - 2, 0), nt):
        for i in range(n):
            for copy in out_copies(k, i):
                copy.wait()


def normalise(where, scale, residual, post_gain, pre_gain, pieces, n, nt):
    rows, width = residual.shape
    block, piece = width // n, rows // nt
    return pl.pallas_call(
        functools.partial(norm_kernel, n, nt),
        out_shape=(
            jax.ShapeDtypeStruct((rows, width), jnp.bfloat16),
            jax.ShapeDtypeStruct((rows, width), jnp.bfloat16),
            jax.ShapeDtypeStruct((3, 8, LANES), jnp.float32),
        ),
        in_specs=[pl.BlockSpec(memory_space=pltpu.SMEM)] * 2
        + [pl.BlockSpec(memory_space=ANY)]
        + [pl.BlockSpec(memory_space=pltpu.VMEM)] * 2
        + [pl.BlockSpec(memory_space=ANY)] * nt,
        out_specs=(
            pl.BlockSpec(memory_space=ANY),
            pl.BlockSpec(memory_space=ANY),
            pl.BlockSpec(memory_space=pltpu.VMEM),
        ),
        scratch_shapes=[
            pltpu.VMEM((2, n, piece, block), jnp.bfloat16),
            pltpu.VMEM((2, n, piece, block), jnp.bfloat16),
            pltpu.VMEM((2, n, piece, block), jnp.bfloat16),
            pltpu.VMEM((2, n, piece, block), jnp.bfloat16),
            pltpu.VMEM((n, ROW_STEP, block), jnp.float32),
            pltpu.SemaphoreType.DMA((2,)),
            pltpu.SemaphoreType.DMA((2, n)),
            pltpu.SemaphoreType.DMA((2, n)),
            pltpu.SemaphoreType.DMA((2, n)),
        ],
        compiler_params=pltpu.CompilerParams(vmem_limit_bytes=VMEM_LIMIT),
        cost_estimate=pl.CostEstimate(
            flops=30 * rows * width, bytes_accessed=8 * rows * width, transcendentals=0
        ),
        name="normalise",
    )(
        where,
        scale,
        residual,
        post_gain.reshape(n, 1, block),
        pre_gain.reshape(n, 1, block),
        *pieces,
    )


def tiled(n, nt, hidden, down_weight, residual, post_gain, pre_gain, cast_scale, amax_history):
    f32, bf16 = jnp.float32, jnp.bfloat16
    place = lax.axis_index("dp")
    member = lax.axis_index("tensor")
    line, pair = place // 2, place % 2
    where = jnp.stack([line, pair, member]).astype(jnp.int32)

    def along(value, step, first, last):
        hops = [
            (z * 2 + p, (z + step) * 2 + p) for z in range(first, last) for p in range(2)
        ]
        return lax.ppermute(value, "dp", hops)

    def over_tensor(value, k):
        return lax.ppermute(value, "tensor", [(t, t ^ k) for t in range(nt)])

    own_w = down_weight.T
    other_w = lax.ppermute(own_w, "dp", [(d, d ^ 1) for d in range(2 * n)])
    halves = 2
    cut = hidden.shape[0] // halves
    parts = [hidden[i * cut : (i + 1) * cut] for i in range(halves)]
    ups, downs = [], []
    up_parts, down_parts = list(parts), list(parts)
    for s in range(1, n):
        up_parts = [along(v, -1, 1, n - s + 1) for v in up_parts]
        down_parts = [along(v, 1, s - 1, n - 1) for v in down_parts]
        ups.append(jnp.concatenate(up_parts, axis=0))
        downs.append(jnp.concatenate(down_parts, axis=0))

    partial = multiply(where, own_w, other_w, hidden, ups, downs, n, nt)

    near = over_tensor(jnp.concatenate([partial[k : k + 1] for k in range(1, nt, 2)]), 1)
    totals = partial[0].astype(f32) + near[0].astype(f32)
    for k in range(2, nt, 2):
        pair_sum = (partial[k].astype(f32) + near[k // 2].astype(f32)).astype(bf16)
        totals = totals + over_tensor(pair_sum, k).astype(f32)
    totals = totals.astype(bf16)

    blocks = []
    for k in range(n):
        mine = lax.dynamic_index_in_dim(totals, lax.rem(line + k, n), 0, keepdims=True)
        if k:
            hops = [(z * 2 + p, (z + k) % n * 2 + p) for z in range(n) for p in range(2)]
            mine = lax.ppermute(mine, "dp", hops)
        blocks.append(mine)
    own_rows = jnp.concatenate(blocks, axis=0)

    pieces = [None] * nt
    pieces[0] = own_rows
    for k in range(2, nt, 2):
        pieces[k] = over_tensor(own_rows, k)
    for k in range(1, nt, 2):
        pieces[k] = over_tensor(pieces[k - 1], 1)

    cast_out, residual_out, peaks = normalise(
        where, cast_scale, residual, post_gain, pre_gain, pieces, n, nt
    )
    peaks = peaks[:, 0, 0]
    bit = 1
    while bit < 2 * n:
        peaks = jnp.maximum(
            peaks, lax.ppermute(peaks, "dp", [(d, d ^ bit) for d in range(2 * n)])
        )
        bit *= 2
    new_history, new_scales = histories(peaks, amax_history)
    return (cast_out, residual_out, peaks, new_history, new_scales)


def power_of_two(value):
    return value & (value - 1) == 0


def solution(mesh):
    ndp, nt = mesh.shape["dp"], mesh.shape["tensor"]

    def on_device(hidden, down_weight, residual, *rest):
        rows, half = hidden.shape[0], down_weight.shape[1]
        fits = (
            ndp >= 4
            and power_of_two(ndp)
            and nt >= 2
            and power_of_two(nt)
            and 2 * half % LANES == 0
            and half % ROW_STEP == 0
            and rows % (nt * ROW_STEP) == 0
            and hidden.shape[1] % LANES == 0
        )
        if fits:
            return tiled(ndp // 2, nt, hidden, down_weight, residual, *rest)
        return general(hidden, down_weight, residual, *rest)

    in_specs = (P("dp", "tensor"), P("tensor", "dp"), P("dp", None), P(), P(), P(), P())
    out_specs = (P("dp", None), P("dp", None), P(), P(), P())
    return jax.shard_map(
        on_device, mesh=mesh, in_specs=in_specs, out_specs=out_specs, check_vma=False
    )
```
